32 devices in a mesh: seq: 8 (over z, y), tensor: 4 (over x, core).
Axes of the slice: x: 2, y: 2, z: 4, core: 2. Of those that a mesh axis runs over, the one named last changes fastest.
Arguments:
- fixed_point: bfloat16 [1024, 4096], P(('seq', 'tensor')), may hold values from -6 to 6
- incoming: bfloat16 [1024, 4096], P(('seq', 'tensor')), may hold values from -6 to 6
- norm_gain: float32 [4096], replicated, may hold values from 0.1 to 1.9
- query_weight: bfloat16 [4096, 4096], P(None, 'tensor'), may hold values from -0.21875 to 0.21875, as said below
- key_weight: bfloat16 [4096, 4096], P(None, 'tensor'), may hold values from -0.265625 to 0.265625, as said below
- value_weight: bfloat16 [4096, 4096], P(None, 'tensor'), may hold values from -0.09375 to 0.09375
- out_weight: bfloat16 [4096, 4096], P('tensor'), may hold values from -0.09375 to 0.09375
- layout: int32 [16, 16], replicated, may hold values 0 or 1
Outputs:
- adjoint: float32 [1024, 4096], P(('seq', 'tensor'))
- gain_grad: float32 [4096], replicated
The draws below stay inside these ranges and needn't reach their ends.
Inputs may be any that keep to these rules, and one draw needn't show every extreme that they name: `query_weight`: entries of the columns of each head are independent; their spread may differ between heads. `key_weight`: entries are independent within a draw; columns of some heads may follow the same head's columns of query_weight. `layout`: A key block strictly before a query block is attended where the entry at row query block, column key block is 1; a block always attends itself causally; entries on or above the diagonal are not read.
All inputs are finite; a program needn't handle non-finite values.
Results may differ from the reference program's by a relative error of at most 0.03.
Values may be sent and summed in bfloat16 or wider, within the bound.
A program may use at most 128 MiB of HBM per device.

```python
import jax
import jax.numpy as jnp
from jax import lax

D = 4096
HEADS = 32
HEAD_DIM = 128
BLK = 64
ITERS = 2
HEADS_DEV = 8
LENGTH = 1024
NBLK = 16


def projection_pair(key):
    first = jax.random.truncated_normal(jax.random.fold_in(key, 11), -4.0, 4.0, (D, D), jnp.float32)
    second = jax.random.truncated_normal(jax.random.fold_in(key, 23), -4.0, 4.0, (D, D), jnp.float32)
    plain = (2.0 / D) ** 0.5
    query = first * plain
    keyed = second * plain
    return (query, keyed)


def draw_query_weight(key, part):
    return projection_pair(key)[0].astype(jnp.bfloat16)


def draw_key_weight(key, part):
    return projection_pair(key)[1].astype(jnp.bfloat16)


def set_ends(values, stream_key, least, top_value):
    shape = values.shape
    place = [jax.random.randint(jax.random.fold_in(stream_key, axis), (), 0, shape[axis]) for axis in range(len(shape))]
    values = values.at[tuple(place)].set(least)
    longest = shape.index(max(shape))
    place[longest] = (place[longest] + 1) % shape[longest]
    return values.at[tuple(place)].set(top_value)


def block_levels(own_key, shape, cuts, smallest, top_value):
    def one(dim, parts):
        heights = jax.random.uniform(jax.random.fold_in(jax.random.fold_in(own_key, 6), dim), (parts,), jnp.float32, smallest / len(cuts), top_value / len(cuts))
        return jnp.repeat(jnp.exp(heights), shape[dim] // parts).reshape((-1,) + (1,) * (len(shape) - dim - 1))

    loudness = one(*cuts[0])
    for cut in cuts[1:]:
        loudness = loudness * one(*cut)
    return loudness


def noise(stream_key, dims, scale, bound, cuts=(), kind=jnp.bfloat16):
    values = scale * jax.random.normal(stream_key, dims, jnp.float32)
    if cuts:
        values = values * block_levels(stream_key, dims, cuts, -0.22, 0.18)
    return jnp.clip(values, -bound, bound).astype(kind)


def setup_inputs(seed: int = 0) -> dict:
    splits = jax.random.split(jax.random.key(seed), 9)
    fixed_point = noise(splits[0], (LENGTH, D), 1.0, 6.0, ((0, 32),))
    incoming = noise(splits[1], (LENGTH, D), 1.0, 6.0, ((0, 32),))
    norm_gain = jnp.clip(1.0 + 0.18 * jax.random.normal(splits[2], (D,), jnp.float32), 0.1, 1.9)
    query_weight = draw_query_weight(jax.random.fold_in(splits[8], 71), 0)
    key_weight = draw_key_weight(jax.random.fold_in(splits[8], 71), 0)
    value_weight = noise(splits[5], (D, D), D ** -0.5, 0.09375, ((1, 4),))
    out_weight = noise(splits[6], (D, D), D ** -0.5, 0.09375, ((0, 4),))
    layout = set_ends((jax.random.randint(splits[7], (NBLK, NBLK), 0, 4) < 3).astype(jnp.int32), jax.random.fold_in(splits[7], 1), 0, 1)
    return dict(fixed_point=fixed_point, incoming=incoming, norm_gain=norm_gain, query_weight=query_weight, key_weight=key_weight, value_weight=value_weight, out_weight=out_weight, layout=layout)


EPS = 1e-05
THETA = 10000.0
MASKED = -1e+30

def round_low(values):
    return lax.optimization_barrier(values.astype(jnp.bfloat16)).astype(jnp.float32)

def rope_tables(positions):
    freq = THETA ** (-jnp.arange(0, HEAD_DIM, 2, dtype=jnp.float32) / HEAD_DIM)
    angle = positions.astype(jnp.float32)[:, None] * freq[None, :]
    cosine = jnp.concatenate([jnp.cos(angle), jnp.cos(angle)], axis=1)[:, None, :]
    sine = jnp.concatenate([jnp.sin(angle), jnp.sin(angle)], axis=1)[:, None, :]
    return (cosine, sine)

def rotate(values, cosine, sine):
    half = HEAD_DIM // 2
    turned = jnp.concatenate([-values[..., half:], values[..., :half]], axis=-1)
    return values * cosine + turned * sine

def rotate_back(values, cosine, sine):
    half = HEAD_DIM // 2
    weighted = values * sine
    turned = jnp.concatenate([weighted[..., half:], -weighted[..., :half]], axis=-1)
    return values * cosine + turned

def expand_blocks(chosen):
    return jnp.repeat(jnp.repeat(chosen, BLK, axis=0), BLK, axis=1)

def pair_mask(query_pos, key_pos, chosen):
    query_block = (query_pos // BLK)[:, None]
    key_block = (key_pos // BLK)[None, :]
    earlier = (key_block < query_block) & chosen
    same = (key_block == query_block) & (key_pos[None, :] <= query_pos[:, None])
    return earlier | same

def reference(fixed_point, incoming, norm_gain, query_weight, key_weight, value_weight, out_weight, layout):
    groups = HEADS // HEADS_DEV
    width = HEADS_DEV * HEAD_DIM
    score_scale = HEAD_DIM ** (-0.5)
    point = fixed_point.astype(jnp.float32)
    inv_rms = lax.rsqrt(lax.optimization_barrier(jnp.mean(point * point, axis=1, keepdims=True)) + EPS)
    scaled = point * inv_rms
    normed = (norm_gain * scaled).astype(jnp.bfloat16)
    positions = jnp.arange(LENGTH, dtype=jnp.int32)
    cosine, sine = rope_tables(positions)

    def project(weight):
        return jnp.dot(normed, weight, preferred_element_type=jnp.float32).reshape(LENGTH, HEADS, HEAD_DIM)

    def split_heads(values):
        return values.reshape(LENGTH, groups, HEADS_DEV, HEAD_DIM).transpose(1, 0, 2, 3)
    queries = split_heads(rotate(project(query_weight), cosine, sine).astype(jnp.bfloat16))
    keys = split_heads(rotate(project(key_weight), cosine, sine).astype(jnp.bfloat16))
    values = split_heads(project(value_weight).astype(jnp.bfloat16))
    allowed = pair_mask(positions, positions, expand_blocks(layout > 0))[None]

    def probabilities(query_group, key_group):
        scores = jnp.einsum('qhd,khd->hqk', query_group.astype(jnp.float32), key_group.astype(jnp.float32)) * score_scale
        scores = jnp.where(allowed, scores, MASKED)
        return jnp.exp(scores - jax.nn.logsumexp(scores, axis=2, keepdims=True))

    def forward_group(operands):
        query_group, key_group, value_group = operands
        probs = probabilities(query_group, key_group)
        attended = jnp.einsum('hqk,khd->qhd', round_low(probs), value_group.astype(jnp.float32))
        return attended.astype(jnp.bfloat16)
    attended = lax.map(forward_group, (queries, keys, values))
    query_cols = query_weight.reshape(D, groups, width).transpose(1, 0, 2)
    key_cols = key_weight.reshape(D, groups, width).transpose(1, 0, 2)
    value_cols = value_weight.reshape(D, groups, width).transpose(1, 0, 2)
    out_rows = out_weight.reshape(groups, width, D)

    def backprop(cotangent):
        cotangent_low = cotangent.astype(jnp.bfloat16)

        def group_step(total, operands):
            query_group, key_group, value_group, attended_group, query_col, key_col, value_col, out_row = operands
            grad_out = jnp.dot(cotangent_low, out_row.T, preferred_element_type=jnp.float32).astype(jnp.bfloat16)
            grad_wide = grad_out.astype(jnp.float32).reshape(LENGTH, HEADS_DEV, HEAD_DIM)
            delta = lax.optimization_barrier(jnp.sum(grad_wide * attended_group.astype(jnp.float32), axis=2)).T
            probs = probabilities(query_group, key_group)
            grad_probs = jnp.einsum('qhd,khd->hqk', grad_wide, value_group.astype(jnp.float32))
            grad_scores = round_low(probs * (grad_probs - delta[:, :, None]))
            grad_query = jnp.einsum('hqk,khd->qhd', grad_scores, key_group.astype(jnp.float32)) * score_scale
            grad_key = jnp.einsum('hqk,qhd->khd', grad_scores, query_group.astype(jnp.float32)) * score_scale
            grad_value = jnp.einsum('hqk,qhd->khd', round_low(probs), grad_wide)
            query_low = rotate_back(grad_query, cosine, sine).astype(jnp.bfloat16).reshape(LENGTH, width)
            key_low = rotate_back(grad_key, cosine, sine).astype(jnp.bfloat16).reshape(LENGTH, width)
            value_low = grad_value.astype(jnp.bfloat16).reshape(LENGTH, width)
            partial_sum = jnp.dot(query_low, query_col.T, preferred_element_type=jnp.float32)
            partial_sum = partial_sum + jnp.dot(key_low, key_col.T, preferred_element_type=jnp.float32)
            partial_sum = partial_sum + jnp.dot(value_low, value_col.T, preferred_element_type=jnp.float32)
            return (total + round_low(partial_sum), None)
        operands = (queries, keys, values, attended, query_cols, key_cols, value_cols, out_rows)
        grad_normed, _ = lax.scan(group_step, jnp.zeros((LENGTH, D), jnp.float32), operands)
        return grad_normed
    cotangent = incoming.astype(jnp.float32)
    adjoint = cotangent
    gain_total = jnp.zeros((D,), jnp.float32)
    for term_index in range(ITERS):
        grad_normed = backprop(cotangent)
        gain_total = gain_total + lax.optimization_barrier(jnp.sum(grad_normed * scaled, axis=0))
        weighted = norm_gain * grad_normed
        inner = lax.optimization_barrier(jnp.sum(weighted * scaled, axis=1, keepdims=True))
        cotangent = inv_rms * (weighted - scaled * (inner / D))
        adjoint = adjoint + cotangent
    return (adjoint, gain_total * LENGTH ** (-0.5))
```

```python
import jax
import jax.numpy as jnp
from jax import lax
from jax.experimental import pallas as pl
from jax.experimental.pallas import tpu as pltpu
from jax.sharding import PartitionSpec as P

HEAD_DIM = 128
BLK = 64
ITERS = 2


EPS = 1e-05
THETA = 10000.0
MASKED = -1e30


def rope_tables(positions):
    freq = THETA ** (-jnp.arange(0, HEAD_DIM, 2, dtype=jnp.float32) / HEAD_DIM)
    angle = positions.astype(jnp.float32)[:, None] * freq[None, :]
    cosine = jnp.concatenate([jnp.cos(angle), jnp.cos(angle)], axis=1)[:, None, :]
    sine = jnp.concatenate([jnp.sin(angle), jnp.sin(angle)], axis=1)[:, None, :]
    return (cosine, sine)


def rotate(values, cosine, sine):
    half = HEAD_DIM // 2
    turned = jnp.concatenate([-values[..., half:], values[..., :half]], axis=-1)
    return values * cosine + turned * sine


def rotate_back(values, cosine, sine):
    half = HEAD_DIM // 2
    weighted = values * sine
    turned = jnp.concatenate([weighted[..., half:], -weighted[..., :half]], axis=-1)
    return values * cosine + turned


def expand_blocks(chosen):
    return jnp.repeat(jnp.repeat(chosen, BLK, axis=0), BLK, axis=1)


def pair_mask(query_pos, key_pos, chosen):
    query_block = (query_pos // BLK)[:, None]
    key_block = (key_pos // BLK)[None, :]
    earlier = (key_block < query_block) & chosen
    same = (key_block == query_block) & (key_pos[None, :] <= query_pos[:, None])
    return earlier | same


def ring_body(
    fixed_point, incoming, norm_gain, query_weight, key_weight, value_weight, out_weight, layout
):
    local_rows, model_width = fixed_point.shape
    head_width = query_weight.shape[1]
    head_count = head_width // HEAD_DIM
    seq_tokens = local_rows * lax.axis_size("tensor")
    seq_length = seq_tokens * lax.axis_size("seq")
    seq_index = lax.axis_index("seq")
    score_scale = HEAD_DIM ** (-0.5)
    contract_last = (((1,), (1,)), ((), ()))
    head_shape = (seq_tokens, head_count, HEAD_DIM)
    point = fixed_point.astype(jnp.float32)
    inv_rms = lax.rsqrt(jnp.mean(point * point, axis=1, keepdims=True) + EPS)
    scaled = point * inv_rms
    normed = (norm_gain * scaled).astype(jnp.bfloat16)
    project_piece = lax.all_gather(normed, "tensor", axis=0, tiled=True)
    projected = jnp.concatenate(
        [
            jnp.dot(project_piece, query_weight, preferred_element_type=jnp.float32),
            jnp.dot(project_piece, key_weight, preferred_element_type=jnp.float32),
            jnp.dot(project_piece, value_weight, preferred_element_type=jnp.float32),
        ],
        axis=1,
    )
    positions = seq_index * seq_tokens + jnp.arange(seq_tokens, dtype=jnp.int32)
    cosine, sine = rope_tables(positions)
    queries = rotate(projected[:, :head_width].reshape(head_shape), cosine, sine).astype(
        jnp.bfloat16
    )
    keys = rotate(
        projected[:, head_width : 2 * head_width].reshape(head_shape), cosine, sine
    ).astype(jnp.bfloat16)
    values = projected[:, 2 * head_width :].reshape(head_shape).astype(jnp.bfloat16)
    block_rows = seq_tokens // BLK
    block_count = seq_length // BLK
    first_block = seq_index * block_rows
    key_positions = jnp.arange(seq_length, dtype=jnp.int32)
    chosen_rows = (
        lax.dynamic_slice(layout, (first_block, jnp.int32(0)), (block_rows, block_count)) > 0
    )
    allowed = pair_mask(positions, key_positions, expand_blocks(chosen_rows))
    keys_all, values_all = (
        lax.all_gather(keys, "seq", axis=0, tiled=True),
        lax.all_gather(values, "seq", axis=0, tiled=True),
    )
    scores = (
        jnp.einsum("qhd,khd->hqk", queries, keys_all, preferred_element_type=jnp.float32)
        * score_scale
    )
    scores = jnp.where(allowed[None], scores, MASKED)
    log_norm = jax.nn.logsumexp(scores, axis=2, keepdims=True)
    probs = jnp.exp(scores - log_norm)
    probs_low = probs.astype(jnp.bfloat16)
    attended = jnp.einsum(
        "hqk,khd->qhd", probs_low, values_all, preferred_element_type=jnp.float32
    ).astype(jnp.bfloat16)
    cotangent = incoming.astype(jnp.float32)
    adjoint = cotangent
    gain_grad = jnp.zeros((model_width,), jnp.float32)
    for term_index in range(ITERS):
        grad_out = lax.dot_general(
            lax.all_gather(cotangent.astype(jnp.bfloat16), "tensor", axis=0, tiled=True),
            out_weight,
            contract_last,
            preferred_element_type=jnp.float32,
        )
        grad_low = grad_out.astype(jnp.bfloat16).reshape(head_shape)
        delta = jnp.sum(grad_low.astype(jnp.float32) * attended.astype(jnp.float32), axis=2)
        grad_probs = jnp.einsum(
            "qhd,khd->hqk", grad_low, values_all, preferred_element_type=jnp.float32
        )
        grad_scores = (probs * (grad_probs - delta.T[:, :, None])).astype(jnp.bfloat16)
        grad_query = (
            jnp.einsum("hqk,khd->qhd", grad_scores, keys_all, preferred_element_type=jnp.float32)
            * score_scale
        )
        key_part = (
            jnp.einsum("hqk,qhd->khd", grad_scores, queries, preferred_element_type=jnp.float32)
            * score_scale
        )
        value_part = jnp.einsum(
            "hqk,qhd->khd", probs_low, grad_low, preferred_element_type=jnp.float32
        )
        key_grads = lax.psum_scatter(
            jnp.concatenate(
                [
                    key_part.reshape(seq_tokens * lax.axis_size("seq"), head_width),
                    value_part.reshape(seq_tokens * lax.axis_size("seq"), head_width),
                ],
                axis=1,
            ).astype(jnp.bfloat16),
            "seq",
            scatter_dimension=0,
            tiled=True,
        ).astype(jnp.float32)
        grad_key = key_grads[:, :head_width].reshape(head_shape)
        grad_value = key_grads[:, head_width:].reshape(head_shape)
        query_low = (
            rotate_back(grad_query, cosine, sine)
            .astype(jnp.bfloat16)
            .reshape(seq_tokens, head_width)
        )
        key_low = (
            rotate_back(grad_key, cosine, sine).astype(jnp.bfloat16).reshape(seq_tokens, head_width)
        )
        value_low = grad_value.astype(jnp.bfloat16).reshape(seq_tokens, head_width)
        total = lax.dot_general(
            query_low, query_weight, contract_last, preferred_element_type=jnp.float32
        )
        total = total + lax.dot_general(
            key_low, key_weight, contract_last, preferred_element_type=jnp.float32
        )
        total = total + lax.dot_general(
            value_low, value_weight, contract_last, preferred_element_type=jnp.float32
        )
        grad_normed = lax.psum_scatter(
            total.astype(jnp.bfloat16), "tensor", scatter_dimension=0, tiled=True
        ).astype(jnp.float32)
        gain_term = jnp.sum(grad_normed * scaled, axis=0)
        gain_grad = gain_grad + lax.psum(gain_term, ("seq", "tensor"))
        weighted = norm_gain * grad_normed
        inner = jnp.sum(weighted * scaled, axis=1, keepdims=True)
        cotangent = inv_rms * (weighted - scaled * (inner / model_width))
        adjoint = adjoint + cotangent
    return (adjoint, gain_grad * seq_length ** (-0.5))


WHOLE, ROWS, COLS = "whole", "rows", "cols"


def block_view(ref, kind, index, count):
    if kind == WHOLE:
        return ref
    if kind == ROWS:
        size = ref.shape[0] // count
        return ref.at[pl.ds(pl.multiple_of(index * size, size), size), :]
    size = ref.shape[1] // count
    return ref.at[:, pl.ds(pl.multiple_of(index * size, size), size)]


def exchange(arrays, kinds, axis, collective_id):
    count = lax.axis_size(axis)
    number = len(arrays)
    shapes = []
    for array, (source, target) in zip(arrays, kinds):
        rows, cols = array.shape
        rows, cols = {WHOLE: (rows, cols), ROWS: (rows // count, cols), COLS: (rows, cols // count)}[source]
        shape = (rows * count, cols) if target == ROWS else (rows, cols * count)
        shapes.append(jax.ShapeDtypeStruct(shape, array.dtype))

    def kernel(*refs):
        sources, results = refs[:number], refs[number : 2 * number]
        send_sem, recv_sem, own_sem = refs[2 * number :]
        me = lax.axis_index(axis)
        barrier = pltpu.get_barrier_semaphore()
        for step in range(1, count):
            pl.semaphore_signal(
                barrier,
                inc=1,
                device_id={axis: lax.rem(me + step, count)},
                device_id_type=pl.DeviceIdType.MESH,
            )
        pl.semaphore_wait(barrier, count - 1)
        copies = []
        for step in range(1, count):
            peer = lax.rem(me + step, count)
            for item, (source, target) in enumerate(kinds):
                copies.append(
                    pltpu.make_async_remote_copy(
                        src_ref=block_view(sources[item], source, peer, count),
                        dst_ref=block_view(results[item], target, me, count),
                        send_sem=send_sem.at[item, step],
                        recv_sem=recv_sem.at[item, step],
                        device_id={axis: peer},
                        device_id_type=pl.DeviceIdType.MESH,
                    )
                )
                copies[-1].start()
        for item, (source, target) in enumerate(kinds):
            copies.append(
                pltpu.make_async_copy(
                    block_view(sources[item], source, me, count),
                    block_view(results[item], target, me, count),
                    own_sem.at[item],
                )
            )
            copies[-1].start()
        for copy in copies:
            copy.wait()

    moved = sum(shape.size * shape.dtype.itemsize for shape in shapes)
    return pl.pallas_call(
        kernel,
        out_shape=shapes,
        in_specs=[pl.BlockSpec(memory_space=pl.ANY)] * number,
        out_specs=[pl.BlockSpec(memory_space=pl.ANY)] * number,
        scratch_shapes=[
            pltpu.SemaphoreType.DMA((number, count)),
            pltpu.SemaphoreType.DMA((number, count)),
            pltpu.SemaphoreType.DMA((number,)),
        ],
        compiler_params=pltpu.CompilerParams(
            collective_id=collective_id, has_side_effects=True, vmem_limit_bytes=1 << 20
        ),
        cost_estimate=pl.CostEstimate(flops=0, bytes_accessed=16 * moved, transcendentals=0),
    )(*arrays)


def sum_blocks(received, count):
    rows = received.shape[0] // count
    total = received[:rows].astype(jnp.float32)
    for index in range(1, count):
        total = total + received[index * rows : (index + 1) * rows].astype(jnp.float32)
    return total


def product(left, right, left_dim, right_dim):
    return lax.dot_general(
        left, right, (((left_dim,), (right_dim,)), ((), ())), preferred_element_type=jnp.float32
    )


def allowed_pairs(layout, length):
    block = jnp.arange(length, dtype=jnp.int32) // BLK
    spread = (block[:, None] == jnp.arange(layout.shape[0], dtype=jnp.int32)[None, :]).astype(
        jnp.bfloat16
    )
    chosen = product(spread, (layout > 0).astype(jnp.bfloat16), 1, 0).astype(jnp.bfloat16)
    chosen = product(chosen, spread, 1, 1) > 0.5
    position = jnp.arange(length, dtype=jnp.int32)
    return pair_mask(position, position, chosen)


def head_body(
    fixed_point, incoming, norm_gain, query_weight, key_weight, value_weight, out_weight, layout
):
    local_rows, model_width = fixed_point.shape
    tensor_count = lax.axis_size("tensor")
    seq_count = lax.axis_size("seq")
    head_width = query_weight.shape[1]
    head_count = head_width // HEAD_DIM
    own_heads = head_count // seq_count
    seq_tokens = local_rows * tensor_count
    seq_length = seq_tokens * seq_count
    score_scale = HEAD_DIM ** (-0.5)
    head_shape = (seq_tokens, head_count, HEAD_DIM)
    point = fixed_point.astype(jnp.float32)
    inv_rms = lax.rsqrt(jnp.mean(point * point, axis=1, keepdims=True) + EPS)
    scaled = point * inv_rms
    normed = (norm_gain * scaled).astype(jnp.bfloat16)
    piece, cotangent_piece = exchange(
        (normed, incoming), ((WHOLE, ROWS), (WHOLE, ROWS)), "tensor", 0
    )
    cosine_all, sine_all = rope_tables(jnp.arange(seq_length, dtype=jnp.int32))
    first = lax.axis_index("seq") * seq_tokens
    cosine = lax.dynamic_slice_in_dim(cosine_all, first, seq_tokens, 0)
    sine = lax.dynamic_slice_in_dim(sine_all, first, seq_tokens, 0)
    cosine_all, sine_all = cosine_all[:, 0], sine_all[:, 0]

    def project(weight):
        return jnp.dot(piece, weight, preferred_element_type=jnp.float32)

    def turned(weight):
        values = rotate(project(weight).reshape(head_shape), cosine, sine)
        return values.astype(jnp.bfloat16).reshape(seq_tokens, head_width)

    grad_first = product(cotangent_piece, out_weight, 1, 1).astype(jnp.bfloat16)
    queries, keys, values, grad_heads = exchange(
        (
            turned(query_weight),
            turned(key_weight),
            project(value_weight).astype(jnp.bfloat16),
            grad_first,
        ),
        ((COLS, ROWS),) * 4,
        "seq",
        1,
    )
    allowed = allowed_pairs(layout, seq_length)
    heads = []
    for head in range(own_heads):
        part = slice(head * HEAD_DIM, (head + 1) * HEAD_DIM)
        query, key, value = queries[:, part], keys[:, part], values[:, part]
        scores = jnp.where(allowed, product(query, key, 1, 1) * score_scale, MASKED)
        probs = jnp.exp(scores - jax.nn.logsumexp(scores, axis=1, keepdims=True))
        probs_low = probs.astype(jnp.bfloat16)
        attended = product(probs_low, value, 1, 0).astype(jnp.bfloat16).astype(jnp.float32)
        heads.append((part, query, key, value, probs, probs_low, attended))
    cotangent = incoming.astype(jnp.float32)
    adjoint = cotangent
    gain_term = jnp.zeros((model_width,), jnp.float32)
    for term_index in range(ITERS):
        base = 2 + 4 * term_index
        if term_index:
            (cotangent_piece,) = exchange(
                (cotangent.astype(jnp.bfloat16),), ((WHOLE, ROWS),), "tensor", base
            )
            (grad_heads,) = exchange(
                (product(cotangent_piece, out_weight, 1, 1).astype(jnp.bfloat16),),
                ((COLS, ROWS),),
                "seq",
                base + 1,
            )
        grads = []
        for part, query, key, value, probs, probs_low, attended in heads:
            grad_low = grad_heads[:, part]
            delta = jnp.sum(grad_low.astype(jnp.float32) * attended, axis=1, keepdims=True)
            grad_probs = product(grad_low, value, 1, 1)
            grad_scores = (probs * (grad_probs - delta)).astype(jnp.bfloat16)
            grad_query = product(grad_scores, key, 1, 0) * score_scale
            grad_key = product(grad_scores, query, 0, 0) * score_scale
            grad_value = product(probs_low, grad_low, 0, 0)
            grads.append(
                (
                    rotate_back(grad_query, cosine_all, sine_all).astype(jnp.bfloat16),
                    rotate_back(grad_key, cosine_all, sine_all).astype(jnp.bfloat16),
                    grad_value.astype(jnp.bfloat16),
                )
            )
        query_low, key_low, value_low = exchange(
            tuple(jnp.concatenate(items, axis=1) for items in zip(*grads)),
            ((ROWS, COLS),) * 3,
            "seq",
            base + 2,
        )
        total = product(query_low, query_weight, 1, 1)
        total = total + product(key_low, key_weight, 1, 1)
        total = total + product(value_low, value_weight, 1, 1)
        (received,) = exchange((total.astype(jnp.bfloat16),), ((ROWS, ROWS),), "tensor", base + 3)
        grad_normed = sum_blocks(received, tensor_count)
        gain_term = gain_term + jnp.sum(grad_normed * scaled, axis=0)
        weighted = norm_gain * grad_normed
        inner = jnp.sum(weighted * scaled, axis=1, keepdims=True)
        cotangent = inv_rms * (weighted - scaled * (inner / model_width))
        adjoint = adjoint + cotangent
    shape = (8, model_width // 8)
    for axis, collective_id in (("tensor", 2 + 4 * ITERS), ("seq", 3 + 4 * ITERS)):
        (received,) = exchange((gain_term.reshape(shape),), ((WHOLE, ROWS),), axis, collective_id)
        gain_term = jnp.sum(received.reshape(-1, *shape), axis=0).reshape(-1)
    return (adjoint, gain_term * seq_length ** (-0.5))


def solution(mesh):
    in_specs = (
        P(("seq", "tensor"), None),
        P(("seq", "tensor"), None),
        P(),
        P(None, "tensor"),
        P(None, "tensor"),
        P(None, "tensor"),
        P("tensor", None),
        P(),
    )
    out_specs = (P(("seq", "tensor"), None), P())
    whole_heads = mesh.shape["tensor"] * mesh.shape["seq"]

    def body(*arrays):
        heads = arrays[3].shape[1] * mesh.shape["tensor"] // HEAD_DIM
        chosen = head_body if heads % whole_heads == 0 else ring_body
        return chosen(*arrays)

    return jax.shard_map(body, mesh=mesh, in_specs=in_specs, out_specs=out_specs, check_vma=False)
```

```python
import jax
import jax.numpy as jnp
from jax import lax
from jax.experimental import pallas as pl
from jax.experimental.pallas import tpu as pltpu
from jax.sharding import PartitionSpec as P

HEAD_DIM = 128
BLK = 64
ITERS = 2


EPS = 1e-05
THETA = 10000.0
MASKED = -1e30


def rope_tables(positions):
    freq = THETA ** (-jnp.arange(0, HEAD_DIM, 2, dtype=jnp.float32) / HEAD_DIM)
    angle = positions.astype(jnp.float32)[:, None] * freq[None, :]
    cosine = jnp.concatenate([jnp.cos(angle), jnp.cos(angle)], axis=1)[:, None, :]
    sine = jnp.concatenate([jnp.sin(angle), jnp.sin(angle)], axis=1)[:, None, :]
    return (cosine, sine)


def rotate(values, cosine, sine):
    half = HEAD_DIM // 2
    turned = jnp.concatenate([-values[..., half:], values[..., :half]], axis=-1)
    return values * cosine + turned * sine


def rotate_back(values, cosine, sine):
    half = HEAD_DIM // 2
    weighted = values * sine
    turned = jnp.concatenate([weighted[..., half:], -weighted[..., :half]], axis=-1)
    return values * cosine + turned


def expand_blocks(chosen):
    return jnp.repeat(jnp.repeat(chosen, BLK, axis=0), BLK, axis=1)


def pair_mask(query_pos, key_pos, chosen):
    query_block = (query_pos // BLK)[:, None]
    key_block = (key_pos // BLK)[None, :]
    earlier = (key_block < query_block) & chosen
    same = (key_block == query_block) & (key_pos[None, :] <= query_pos[:, None])
    return earlier | same


def ring_body(
    fixed_point, incoming, norm_gain, query_weight, key_weight, value_weight, out_weight, layout
):
    local_rows, model_width = fixed_point.shape
    head_width = query_weight.shape[1]
    head_count = head_width // HEAD_DIM
    seq_tokens = local_rows * lax.axis_size("tensor")
    seq_length = seq_tokens * lax.axis_size("seq")
    seq_index = lax.axis_index("seq")
    score_scale = HEAD_DIM ** (-0.5)
    contract_last = (((1,), (1,)), ((), ()))
    head_shape = (seq_tokens, head_count, HEAD_DIM)
    point = fixed_point.astype(jnp.float32)
    inv_rms = lax.rsqrt(jnp.mean(point * point, axis=1, keepdims=True) + EPS)
    scaled = point * inv_rms
    normed = (norm_gain * scaled).astype(jnp.bfloat16)
    project_piece = lax.all_gather(normed, "tensor", axis=0, tiled=True)
    projected = jnp.concatenate(
        [
            jnp.dot(project_piece, query_weight, preferred_element_type=jnp.float32),
            jnp.dot(project_piece, key_weight, preferred_element_type=jnp.float32),
            jnp.dot(project_piece, value_weight, preferred_element_type=jnp.float32),
        ],
        axis=1,
    )
    positions = seq_index * seq_tokens + jnp.arange(seq_tokens, dtype=jnp.int32)
    cosine, sine = rope_tables(positions)
    queries = rotate(projected[:, :head_width].reshape(head_shape), cosine, sine).astype(
        jnp.bfloat16
    )
    keys = rotate(
        projected[:, head_width : 2 * head_width].reshape(head_shape), cosine, sine
    ).astype(jnp.bfloat16)
    values = projected[:, 2 * head_width :].reshape(head_shape).astype(jnp.bfloat16)
    block_rows = seq_tokens // BLK
    block_count = seq_length // BLK
    first_block = seq_index * block_rows
    key_positions = jnp.arange(seq_length, dtype=jnp.int32)
    chosen_rows = (
        lax.dynamic_slice(layout, (first_block, jnp.int32(0)), (block_rows, block_count)) > 0
    )
    allowed = pair_mask(positions, key_positions, expand_blocks(chosen_rows))
    keys_all, values_all = (
        lax.all_gather(keys, "seq", axis=0, tiled=True),
        lax.all_gather(values, "seq", axis=0, tiled=True),
    )
    scores = (
        jnp.einsum("qhd,khd->hqk", queries, keys_all, preferred_element_type=jnp.float32)
        * score_scale
    )
    scores = jnp.where(allowed[None], scores, MASKED)
    log_norm = jax.nn.logsumexp(scores, axis=2, keepdims=True)
    probs = jnp.exp(scores - log_norm)
    probs_low = probs.astype(jnp.bfloat16)
    attended = jnp.einsum(
        "hqk,khd->qhd", probs_low, values_all, preferred_element_type=jnp.float32
    ).astype(jnp.bfloat16)
    cotangent = incoming.astype(jnp.float32)
    adjoint = cotangent
    gain_grad = jnp.zeros((model_width,), jnp.float32)
    for term_index in range(ITERS):
        grad_out = lax.dot_general(
            lax.all_gather(cotangent.astype(jnp.bfloat16), "tensor", axis=0, tiled=True),
            out_weight,
            contract_last,
            preferred_element_type=jnp.float32,
        )
        grad_low = grad_out.astype(jnp.bfloat16).reshape(head_shape)
        delta = jnp.sum(grad_low.astype(jnp.float32) * attended.astype(jnp.float32), axis=2)
        grad_probs = jnp.einsum(
            "qhd,khd->hqk", grad_low, values_all, preferred_element_type=jnp.float32
        )
        grad_scores = (probs * (grad_probs - delta.T[:, :, None])).astype(jnp.bfloat16)
        grad_query = (
            jnp.einsum("hqk,khd->qhd", grad_scores, keys_all, preferred_element_type=jnp.float32)
            * score_scale
        )
        key_part = (
            jnp.einsum("hqk,qhd->khd", grad_scores, queries, preferred_element_type=jnp.float32)
            * score_scale
        )
        value_part = jnp.einsum(
            "hqk,qhd->khd", probs_low, grad_low, preferred_element_type=jnp.float32
        )
        key_grads = lax.psum_scatter(
            jnp.concatenate(
                [
                    key_part.reshape(seq_tokens * lax.axis_size("seq"), head_width),
                    value_part.reshape(seq_tokens * lax.axis_size("seq"), head_width),
                ],
                axis=1,
            ).astype(jnp.bfloat16),
            "seq",
            scatter_dimension=0,
            tiled=True,
        ).astype(jnp.float32)
        grad_key = key_grads[:, :head_width].reshape(head_shape)
        grad_value = key_grads[:, head_width:].reshape(head_shape)
        query_low = (
            rotate_back(grad_query, cosine, sine)
            .astype(jnp.bfloat16)
            .reshape(seq_tokens, head_width)
        )
        key_low = (
            rotate_back(grad_key, cosine, sine).astype(jnp.bfloat16).reshape(seq_tokens, head_width)
        )
        value_low = grad_value.astype(jnp.bfloat16).reshape(seq_tokens, head_width)
        total = lax.dot_general(
            query_low, query_weight, contract_last, preferred_element_type=jnp.float32
        )
        total = total + lax.dot_general(
            key_low, key_weight, contract_last, preferred_element_type=jnp.float32
        )
        total = total + lax.dot_general(
            value_low, value_weight, contract_last, preferred_element_type=jnp.float32
        )
        grad_normed = lax.psum_scatter(
            total.astype(jnp.bfloat16), "tensor", scatter_dimension=0, tiled=True
        ).astype(jnp.float32)
        gain_term = jnp.sum(grad_normed * scaled, axis=0)
        gain_grad = gain_grad + lax.psum(gain_term, ("seq", "tensor"))
        weighted = norm_gain * grad_normed
        inner = jnp.sum(weighted * scaled, axis=1, keepdims=True)
        cotangent = inv_rms * (weighted - scaled * (inner / model_width))
        adjoint = adjoint + cotangent
    return (adjoint, gain_grad * seq_length ** (-0.5))


WHOLE, ROWS, COLS = "whole", "rows", "cols"
COMM_BYTES = 80 << 20


def block_view(ref, kind, index, count):
    if kind == WHOLE:
        return ref
    if kind == ROWS:
        size = ref.shape[0] // count
        return ref.at[pl.ds(pl.multiple_of(index * size, size), size), :]
    size = ref.shape[1] // count
    return ref.at[:, pl.ds(pl.multiple_of(index * size, size), size)]


def exchange(arrays, kinds, axis, collective_id):
    count = lax.axis_size(axis)
    number = len(arrays)
    shapes = []
    for array, (source, target) in zip(arrays, kinds):
        rows, cols = array.shape
        rows, cols = {WHOLE: (rows, cols), ROWS: (rows // count, cols), COLS: (rows, cols // count)}[source]
        shape = (rows * count, cols) if target == ROWS else (rows, cols * count)
        shapes.append(jax.ShapeDtypeStruct(shape, array.dtype))

    def kernel(*refs):
        sources, results = refs[:number], refs[number : 2 * number]
        send_sem, recv_sem, own_sem = refs[2 * number :]
        me = lax.axis_index(axis)
        barrier = pltpu.get_barrier_semaphore()
        for step in range(1, count):
            pl.semaphore_signal(
                barrier,
                inc=1,
                device_id={axis: lax.rem(me + step, count)},
                device_id_type=pl.DeviceIdType.MESH,
            )
        pl.semaphore_wait(barrier, count - 1)
        copies = []
        for step in range(1, count):
            peer = lax.rem(me + step, count)
            for item, (source, target) in enumerate(kinds):
                copies.append(
                    pltpu.make_async_remote_copy(
                        src_ref=block_view(sources[item], source, peer, count),
                        dst_ref=block_view(results[item], target, me, count),
                        send_sem=send_sem.at[item, step],
                        recv_sem=recv_sem.at[item, step],
                        device_id={axis: peer},
                        device_id_type=pl.DeviceIdType.MESH,
                    )
                )
                copies[-1].start()
        for item, (source, target) in enumerate(kinds):
            copies.append(
                pltpu.make_async_copy(
                    block_view(sources[item], source, me, count),
                    block_view(results[item], target, me, count),
                    own_sem.at[item],
                )
            )
            copies[-1].start()
        for copy in copies:
            copy.wait()

    moved = sum(shape.size * shape.dtype.itemsize for shape in shapes)
    return pl.pallas_call(
        kernel,
        out_shape=shapes,
        in_specs=[pl.BlockSpec(memory_space=pl.ANY)] * number,
        out_specs=[pl.BlockSpec(memory_space=pl.ANY)] * number,
        scratch_shapes=[
            pltpu.SemaphoreType.DMA((number, count)),
            pltpu.SemaphoreType.DMA((number, count)),
            pltpu.SemaphoreType.DMA((number,)),
        ],
        compiler_params=pltpu.CompilerParams(
            collective_id=collective_id, has_side_effects=True, vmem_limit_bytes=1 << 20
        ),
        cost_estimate=pl.CostEstimate(flops=0, bytes_accessed=COMM_BYTES, transcendentals=0),
    )(*arrays)


def chip_gather(arrays, axis, collective_id):
    count = lax.axis_size(axis)
    number = len(arrays)
    shapes = [jax.ShapeDtypeStruct((a.shape[0] * count, a.shape[1]), a.dtype) for a in arrays]

    def kernel(*refs):
        sources, results = refs[:number], refs[number : 2 * number]
        send_sem, recv_sem, own_sem = refs[2 * number :]
        me = lax.axis_index(axis)
        partner = me + 1 - 2 * lax.rem(me, 2)
        barrier = pltpu.get_barrier_semaphore()
        for peer in [partner] + [lax.rem(me + step, count) for step in range(2, count, 2)]:
            pl.semaphore_signal(
                barrier, inc=1, device_id={axis: peer}, device_id_type=pl.DeviceIdType.MESH
            )
        pl.semaphore_wait(barrier, count // 2)

        def send(item, source, block, peer, slot):
            copy = pltpu.make_async_remote_copy(
                src_ref=source,
                dst_ref=block_view(results[item], ROWS, block, count),
                send_sem=send_sem.at[item, slot],
                recv_sem=recv_sem.at[item, slot],
                device_id={axis: peer},
                device_id_type=pl.DeviceIdType.MESH,
            )
            copy.start()
            return copy

        far, near, own = [], [], []
        for item in range(number):
            for step in range(2, count, 2):
                peer = lax.rem(me + step, count)
                far.append((item, step, send(item, sources[item], me, peer, step)))
        for item in range(number):
            near.append(send(item, sources[item], me, partner, 1))
            own.append(
                pltpu.make_async_copy(
                    sources[item], block_view(results[item], ROWS, me, count), own_sem.at[item]
                )
            )
            own[-1].start()
        for item, step, copy in far:
            copy.wait_recv()
            origin = lax.rem(me - step + count, count)
            block = block_view(results[item], ROWS, origin, count)
            near.append(send(item, block, origin, partner, step + 1))
        for item, step, copy in far:
            copy.wait_send()
        for copy in near + own:
            copy.wait()

    return pl.pallas_call(
        kernel,
        out_shape=shapes,
        in_specs=[pl.BlockSpec(memory_space=pl.ANY)] * number,
        out_specs=[pl.BlockSpec(memory_space=pl.ANY)] * number,
        scratch_shapes=[
            pltpu.SemaphoreType.DMA((number, count)),
            pltpu.SemaphoreType.DMA((number, count)),
            pltpu.SemaphoreType.DMA((number,)),
        ],
        compiler_params=pltpu.CompilerParams(
            collective_id=collective_id, has_side_effects=True, vmem_limit_bytes=1 << 20
        ),
        cost_estimate=pl.CostEstimate(flops=0, bytes_accessed=COMM_BYTES, transcendentals=0),
    )(*arrays)


def chip_scatter(total, axis, collective_id):
    count = lax.axis_size(axis)
    chips = count // 2
    rows, cols = total.shape[0] // count, total.shape[1]
    shape = (chips * rows, cols)

    def kernel(total_ref, result, handed, sums, near_send, near_recv, far_send, far_recv):
        me = lax.axis_index(axis)
        core = lax.rem(me, 2)
        chip = lax.div(me, 2)
        partner = me + 1 - 2 * core
        barrier = pltpu.get_barrier_semaphore()
        for peer in [partner] + [lax.rem(me + step, count) for step in range(2, count, 2)]:
            pl.semaphore_signal(
                barrier, inc=1, device_id={axis: peer}, device_id_type=pl.DeviceIdType.MESH
            )
        pl.semaphore_wait(barrier, chips)
        order = list(range(1, chips)) + [0]
        near, far = [], []
        for step in order:
            target = lax.rem(chip + step, chips)
            copy = pltpu.make_async_remote_copy(
                src_ref=block_view(total_ref, ROWS, 2 * target + 1 - core, count),
                dst_ref=handed.at[pl.ds(step * rows, rows), :],
                send_sem=near_send.at[step],
                recv_sem=near_recv.at[step],
                device_id={axis: partner},
                device_id_type=pl.DeviceIdType.MESH,
            )
            copy.start()
            near.append(copy)
        for step, arrived in zip(order, near):
            arrived.wait_recv()
            target = lax.rem(chip + step, chips)
            place = pl.ds(step * rows, rows)
            own = block_view(total_ref, ROWS, 2 * target + core, count)[...]
            pair = own.astype(jnp.float32) + handed[place, :].astype(jnp.float32)
            if step == 0:
                result[pl.ds(pl.multiple_of(chip * rows, rows), rows), :] = pair.astype(result.dtype)
                continue
            sums[place, :] = pair.astype(sums.dtype)
            copy = pltpu.make_async_remote_copy(
                src_ref=sums.at[place, :],
                dst_ref=block_view(result, ROWS, chip, chips),
                send_sem=far_send.at[step],
                recv_sem=far_recv.at[step],
                device_id={axis: 2 * target + core},
                device_id_type=pl.DeviceIdType.MESH,
            )
            copy.start()
            far.append(copy)
        for copy in near:
            copy.wait_send()
        for copy in far:
            copy.wait()

    return pl.pallas_call(
        kernel,
        out_shape=jax.ShapeDtypeStruct(shape, total.dtype),
        in_specs=[pl.BlockSpec(memory_space=pltpu.VMEM)],
        out_specs=pl.BlockSpec(memory_space=pltpu.VMEM),
        scratch_shapes=[
            pltpu.VMEM(shape, total.dtype),
            pltpu.VMEM(shape, total.dtype),
            pltpu.SemaphoreType.DMA((chips,)),
            pltpu.SemaphoreType.DMA((chips,)),
            pltpu.SemaphoreType.DMA((chips,)),
            pltpu.SemaphoreType.DMA((chips,)),
        ],
        compiler_params=pltpu.CompilerParams(
            collective_id=collective_id, has_side_effects=True, vmem_limit_bytes=8 << 20
        ),
        cost_estimate=pl.CostEstimate(flops=0, bytes_accessed=COMM_BYTES, transcendentals=0),
    )(total)


def sum_blocks(received, count):
    rows = received.shape[0] // count
    total = received[:rows].astype(jnp.float32)
    for index in range(1, count):
        total = total + received[index * rows : (index + 1) * rows].astype(jnp.float32)
    return total


def product(left, right, left_dim, right_dim):
    return lax.dot_general(
        left, right, (((left_dim,), (right_dim,)), ((), ())), preferred_element_type=jnp.float32
    )


def allowed_pairs(layout, length):
    block = jnp.arange(length, dtype=jnp.int32) // BLK
    spread = (block[:, None] == jnp.arange(layout.shape[0], dtype=jnp.int32)[None, :]).astype(
        jnp.bfloat16
    )
    chosen = product(spread, (layout > 0).astype(jnp.bfloat16), 1, 0).astype(jnp.bfloat16)
    chosen = product(chosen, spread, 1, 1) > 0.5
    position = jnp.arange(length, dtype=jnp.int32)
    return pair_mask(position, position, chosen)


def head_body(
    fixed_point, incoming, norm_gain, query_weight, key_weight, value_weight, out_weight, layout
):
    local_rows, model_width = fixed_point.shape
    tensor_count = lax.axis_size("tensor")
    seq_count = lax.axis_size("seq")
    head_width = query_weight.shape[1]
    head_count = head_width // HEAD_DIM
    own_heads = head_count // seq_count
    seq_tokens = local_rows * tensor_count
    seq_length = seq_tokens * seq_count
    score_scale = HEAD_DIM ** (-0.5)
    head_shape = (seq_tokens, head_count, HEAD_DIM)
    point = fixed_point.astype(jnp.float32)
    inv_rms = lax.rsqrt(jnp.mean(point * point, axis=1, keepdims=True) + EPS)
    scaled = point * inv_rms
    normed = (norm_gain * scaled).astype(jnp.bfloat16)
    piece, cotangent_piece = chip_gather((normed, incoming), "tensor", 0)
    cosine_all, sine_all = rope_tables(jnp.arange(seq_length, dtype=jnp.int32))
    first = lax.axis_index("seq") * seq_tokens
    cosine = lax.dynamic_slice_in_dim(cosine_all, first, seq_tokens, 0)
    sine = lax.dynamic_slice_in_dim(sine_all, first, seq_tokens, 0)
    cosine_all, sine_all = cosine_all[:, 0], sine_all[:, 0]

    def project(weight):
        return jnp.dot(piece, weight, preferred_element_type=jnp.float32)

    def turned(weight):
        values = rotate(project(weight).reshape(head_shape), cosine, sine)
        return values.astype(jnp.bfloat16).reshape(seq_tokens, head_width)

    grad_first = product(cotangent_piece, out_weight, 1, 1).astype(jnp.bfloat16)
    queries, keys, values, grad_heads = exchange(
        (
            turned(query_weight),
            turned(key_weight),
            project(value_weight).astype(jnp.bfloat16),
            grad_first,
        ),
        ((COLS, ROWS),) * 4,
        "seq",
        1,
    )
    allowed = allowed_pairs(layout, seq_length)
    heads = []
    for head in range(own_heads):
        part = slice(head * HEAD_DIM, (head + 1) * HEAD_DIM)
        query, key, value = queries[:, part], keys[:, part], values[:, part]
        scores = jnp.where(allowed, product(query, key, 1, 1) * score_scale, MASKED)
        probs = jnp.exp(scores - jax.nn.logsumexp(scores, axis=1, keepdims=True))
        probs_low = probs.astype(jnp.bfloat16)
        attended = product(probs_low, value, 1, 0).astype(jnp.bfloat16).astype(jnp.float32)
        heads.append((part, query, key, value, probs, probs_low, attended))
    cotangent = incoming.astype(jnp.float32)
    adjoint = cotangent
    gain_term = jnp.zeros((model_width,), jnp.float32)
    for term_index in range(ITERS):
        base = 2 + 4 * term_index
        if term_index:
            (cotangent_piece,) = chip_gather((cotangent.astype(jnp.bfloat16),), "tensor", base)
            (grad_heads,) = exchange(
                (product(cotangent_piece, out_weight, 1, 1).astype(jnp.bfloat16),),
                ((COLS, ROWS),),
                "seq",
                base + 1,
            )
        grads = []
        for part, query, key, value, probs, probs_low, attended in heads:
            grad_low = grad_heads[:, part]
            delta = jnp.sum(grad_low.astype(jnp.float32) * attended, axis=1, keepdims=True)
            grad_probs = product(grad_low, value, 1, 1)
            grad_scores = (probs * (grad_probs - delta)).astype(jnp.bfloat16)
            grad_query = product(grad_scores, key, 1, 0) * score_scale
            grad_key = product(grad_scores, query, 0, 0) * score_scale
            grad_value = product(probs_low, grad_low, 0, 0)
            grads.append(
                (
                    rotate_back(grad_query, cosine_all, sine_all).astype(jnp.bfloat16),
                    rotate_back(grad_key, cosine_all, sine_all).astype(jnp.bfloat16),
                    grad_value.astype(jnp.bfloat16),
                )
            )
        query_low, key_low, value_low = exchange(
            tuple(jnp.concatenate(items, axis=1) for items in zip(*grads)),
            ((ROWS, COLS),) * 3,
            "seq",
            base + 2,
        )
        total = product(query_low, query_weight, 1, 1)
        total = total + product(key_low, key_weight, 1, 1)
        total = total + product(value_low, value_weight, 1, 1)
        received = chip_scatter(total.astype(jnp.bfloat16), "tensor", base + 3)
        grad_normed = sum_blocks(received, tensor_count // 2)
        gain_term = gain_term + jnp.sum(grad_normed * scaled, axis=0)
        weighted = norm_gain * grad_normed
        inner = jnp.sum(weighted * scaled, axis=1, keepdims=True)
        cotangent = inv_rms * (weighted - scaled * (inner / model_width))
        adjoint = adjoint + cotangent
    shape = (8, model_width // 8)
    for axis, collective_id in (("tensor", 2 + 4 * ITERS), ("seq", 3 + 4 * ITERS)):
        (received,) = exchange((gain_term.reshape(shape),), ((WHOLE, ROWS),), axis, collective_id)
        gain_term = jnp.sum(received.reshape(-1, *shape), axis=0).reshape(-1)
    return (adjoint, gain_term * seq_length ** (-0.5))


def solution(mesh):
    in_specs = (
        P(("seq", "tensor"), None),
        P(("seq", "tensor"), None),
        P(),
        P(None, "tensor"),
        P(None, "tensor"),
        P(None, "tensor"),
        P("tensor", None),
        P(),
    )
    out_specs = (P(("seq", "tensor"), None), P())
    whole_heads = mesh.shape["tensor"] * mesh.shape["seq"]

    def body(*arrays):
        heads = arrays[3].shape[1] * mesh.shape["tensor"] // HEAD_DIM
        even = mesh.shape["tensor"] % 2 == 0
        chosen = head_body if even and heads % whole_heads == 0 else ring_body
        return chosen(*arrays)

    return jax.shard_map(body, mesh=mesh, in_specs=in_specs, out_specs=out_specs, check_vma=False)
```

```python
import jax
import jax.numpy as jnp
from jax import lax
from jax.experimental import pallas as pl
from jax.experimental.pallas import tpu as pltpu
from jax.sharding import PartitionSpec as P

HEAD_DIM = 128
BLK = 64
ITERS = 2


EPS = 1e-05
THETA = 10000.0
MASKED = -1e30


def rope_tables(positions):
    freq = THETA ** (-jnp.arange(0, HEAD_DIM, 2, dtype=jnp.float32) / HEAD_DIM)
    angle = positions.astype(jnp.float32)[:, None] * freq[None, :]
    cosine = jnp.concatenate([jnp.cos(angle), jnp.cos(angle)], axis=1)[:, None, :]
    sine = jnp.concatenate([jnp.sin(angle), jnp.sin(angle)], axis=1)[:, None, :]
    return (cosine, sine)


def rotate(values, cosine, sine):
    half = HEAD_DIM // 2
    turned = jnp.concatenate([-values[..., half:], values[..., :half]], axis=-1)
    return values * cosine + turned * sine


def rotate_back(values, cosine, sine):
    half = HEAD_DIM // 2
    weighted = values * sine
    turned = jnp.concatenate([weighted[..., half:], -weighted[..., :half]], axis=-1)
    return values * cosine + turned


def expand_blocks(chosen):
    return jnp.repeat(jnp.repeat(chosen, BLK, axis=0), BLK, axis=1)


def pair_mask(query_pos, key_pos, chosen):
    query_block = (query_pos // BLK)[:, None]
    key_block = (key_pos // BLK)[None, :]
    earlier = (key_block < query_block) & chosen
    same = (key_block == query_block) & (key_pos[None, :] <= query_pos[:, None])
    return earlier | same


def ring_body(
    fixed_point, incoming, norm_gain, query_weight, key_weight, value_weight, out_weight, layout
):
    local_rows, model_width = fixed_point.shape
    head_width = query_weight.shape[1]
    head_count = head_width // HEAD_DIM
    seq_tokens = local_rows * lax.axis_size("tensor")
    seq_length = seq_tokens * lax.axis_size("seq")
    seq_index = lax.axis_index("seq")
    score_scale = HEAD_DIM ** (-0.5)
    contract_last = (((1,), (1,)), ((), ()))
    head_shape = (seq_tokens, head_count, HEAD_DIM)
    point = fixed_point.astype(jnp.float32)
    inv_rms = lax.rsqrt(jnp.mean(point * point, axis=1, keepdims=True) + EPS)
    scaled = point * inv_rms
    normed = (norm_gain * scaled).astype(jnp.bfloat16)
    project_piece = lax.all_gather(normed, "tensor", axis=0, tiled=True)
    projected = jnp.concatenate(
        [
            jnp.dot(project_piece, query_weight, preferred_element_type=jnp.float32),
            jnp.dot(project_piece, key_weight, preferred_element_type=jnp.float32),
            jnp.dot(project_piece, value_weight, preferred_element_type=jnp.float32),
        ],
        axis=1,
    )
    positions = seq_index * seq_tokens + jnp.arange(seq_tokens, dtype=jnp.int32)
    cosine, sine = rope_tables(positions)
    queries = rotate(projected[:, :head_width].reshape(head_shape), cosine, sine).astype(
        jnp.bfloat16
    )
    keys = rotate(
        projected[:, head_width : 2 * head_width].reshape(head_shape), cosine, sine
    ).astype(jnp.bfloat16)
    values = projected[:, 2 * head_width :].reshape(head_shape).astype(jnp.bfloat16)
    block_rows = seq_tokens // BLK
    block_count = seq_length // BLK
    first_block = seq_index * block_rows
    key_positions = jnp.arange(seq_length, dtype=jnp.int32)
    chosen_rows = (
        lax.dynamic_slice(layout, (first_block, jnp.int32(0)), (block_rows, block_count)) > 0
    )
    allowed = pair_mask(positions, key_positions, expand_blocks(chosen_rows))
    keys_all, values_all = (
        lax.all_gather(keys, "seq", axis=0, tiled=True),
        lax.all_gather(values, "seq", axis=0, tiled=True),
    )
    scores = (
        jnp.einsum("qhd,khd->hqk", queries, keys_all, preferred_element_type=jnp.float32)
        * score_scale
    )
    scores = jnp.where(allowed[None], scores, MASKED)
    log_norm = jax.nn.logsumexp(scores, axis=2, keepdims=True)
    probs = jnp.exp(scores - log_norm)
    probs_low = probs.astype(jnp.bfloat16)
    attended = jnp.einsum(
        "hqk,khd->qhd", probs_low, values_all, preferred_element_type=jnp.float32
    ).astype(jnp.bfloat16)
    cotangent = incoming.astype(jnp.float32)
    adjoint = cotangent
    gain_grad = jnp.zeros((model_width,), jnp.float32)
    for term_index in range(ITERS):
        grad_out = lax.dot_general(
            lax.all_gather(cotangent.astype(jnp.bfloat16), "tensor", axis=0, tiled=True),
            out_weight,
            contract_last,
            preferred_element_type=jnp.float32,
        )
        grad_low = grad_out.astype(jnp.bfloat16).reshape(head_shape)
        delta = jnp.sum(grad_low.astype(jnp.float32) * attended.astype(jnp.float32), axis=2)
        grad_probs = jnp.einsum(
            "qhd,khd->hqk", grad_low, values_all, preferred_element_type=jnp.float32
        )
        grad_scores = (probs * (grad_probs - delta.T[:, :, None])).astype(jnp.bfloat16)
        grad_query = (
            jnp.einsum("hqk,khd->qhd", grad_scores, keys_all, preferred_element_type=jnp.float32)
            * score_scale
        )
        key_part = (
            jnp.einsum("hqk,qhd->khd", grad_scores, queries, preferred_element_type=jnp.float32)
            * score_scale
        )
        value_part = jnp.einsum(
            "hqk,qhd->khd", probs_low, grad_low, preferred_element_type=jnp.float32
        )
        key_grads = lax.psum_scatter(
            jnp.concatenate(
                [
                    key_part.reshape(seq_tokens * lax.axis_size("seq"), head_width),
                    value_part.reshape(seq_tokens * lax.axis_size("seq"), head_width),
                ],
                axis=1,
            ).astype(jnp.bfloat16),
            "seq",
            scatter_dimension=0,
            tiled=True,
        ).astype(jnp.float32)
        grad_key = key_grads[:, :head_width].reshape(head_shape)
        grad_value = key_grads[:, head_width:].reshape(head_shape)
        query_low = (
            rotate_back(grad_query, cosine, sine)
            .astype(jnp.bfloat16)
            .reshape(seq_tokens, head_width)
        )
        key_low = (
            rotate_back(grad_key, cosine, sine).astype(jnp.bfloat16).reshape(seq_tokens, head_width)
        )
        value_low = grad_value.astype(jnp.bfloat16).reshape(seq_tokens, head_width)
        total = lax.dot_general(
            query_low, query_weight, contract_last, preferred_element_type=jnp.float32
        )
        total = total + lax.dot_general(
            key_low, key_weight, contract_last, preferred_element_type=jnp.float32
        )
        total = total + lax.dot_general(
            value_low, value_weight, contract_last, preferred_element_type=jnp.float32
        )
        grad_normed = lax.psum_scatter(
            total.astype(jnp.bfloat16), "tensor", scatter_dimension=0, tiled=True
        ).astype(jnp.float32)
        gain_term = jnp.sum(grad_normed * scaled, axis=0)
        gain_grad = gain_grad + lax.psum(gain_term, ("seq", "tensor"))
        weighted = norm_gain * grad_normed
        inner = jnp.sum(weighted * scaled, axis=1, keepdims=True)
        cotangent = inv_rms * (weighted - scaled * (inner / model_width))
        adjoint = adjoint + cotangent
    return (adjoint, gain_grad * seq_length ** (-0.5))


WHOLE, ROWS, COLS = "whole", "rows", "cols"
COMM_BYTES = 80 << 20


def block_view(ref, kind, index, count):
    if kind == WHOLE:
        return ref
    if kind == ROWS:
        size = ref.shape[0] // count
        return ref.at[pl.ds(pl.multiple_of(index * size, size), size), :]
    size = ref.shape[1] // count
    return ref.at[:, pl.ds(pl.multiple_of(index * size, size), size)]


def exchange(arrays, kinds, axis, collective_id):
    count = lax.axis_size(axis)
    number = len(arrays)
    shapes = []
    for array, (source, target) in zip(arrays, kinds):
        rows, cols = array.shape
        rows, cols = {WHOLE: (rows, cols), ROWS: (rows // count, cols), COLS: (rows, cols // count)}[source]
        shape = (rows * count, cols) if target == ROWS else (rows, cols * count)
        shapes.append(jax.ShapeDtypeStruct(shape, array.dtype))

    def kernel(*refs):
        sources, results = refs[:number], refs[number : 2 * number]
        send_sem, recv_sem, own_sem = refs[2 * number :]
        me = lax.axis_index(axis)
        barrier = pltpu.get_barrier_semaphore()
        for step in range(1, count):
            pl.semaphore_signal(
                barrier,
                inc=1,
                device_id={axis: lax.rem(me + step, count)},
                device_id_type=pl.DeviceIdType.MESH,
            )
        pl.semaphore_wait(barrier, count - 1)
        copies = []
        for step in range(1, count):
            peer = lax.rem(me + step, count)
            for item, (source, target) in enumerate(kinds):
                copies.append(
                    pltpu.make_async_remote_copy(
                        src_ref=block_view(sources[item], source, peer, count),
                        dst_ref=block_view(results[item], target, me, count),
                        send_sem=send_sem.at[item, step],
                        recv_sem=recv_sem.at[item, step],
                        device_id={axis: peer},
                        device_id_type=pl.DeviceIdType.MESH,
                    )
                )
                copies[-1].start()
        for item, (source, target) in enumerate(kinds):
            copies.append(
                pltpu.make_async_copy(
                    block_view(sources[item], source, me, count),
                    block_view(results[item], target, me, count),
                    own_sem.at[item],
                )
            )
            copies[-1].start()
        for copy in copies:
            copy.wait()

    moved = sum(shape.size * shape.dtype.itemsize for shape in shapes)
    return pl.pallas_call(
        kernel,
        out_shape=shapes,
        in_specs=[pl.BlockSpec(memory_space=pl.ANY)] * number,
        out_specs=[pl.BlockSpec(memory_space=pl.ANY)] * number,
        scratch_shapes=[
            pltpu.SemaphoreType.DMA((number, count)),
            pltpu.SemaphoreType.DMA((number, count)),
            pltpu.SemaphoreType.DMA((number,)),
        ],
        compiler_params=pltpu.CompilerParams(
            collective_id=collective_id, has_side_effects=True, vmem_limit_bytes=1 << 20
        ),
        cost_estimate=pl.CostEstimate(flops=0, bytes_accessed=COMM_BYTES, transcendentals=0),
    )(*arrays)


def chip_gather(arrays, axis, collective_id):
    count = lax.axis_size(axis)
    number = len(arrays)
    shapes = [jax.ShapeDtypeStruct((a.shape[0] * count, a.shape[1]), a.dtype) for a in arrays]

    def kernel(*refs):
        sources, results = refs[:number], refs[number : 2 * number]
        send_sem, recv_sem, own_sem = refs[2 * number :]
        me = lax.axis_index(axis)
        partner = me + 1 - 2 * lax.rem(me, 2)
        barrier = pltpu.get_barrier_semaphore()
        for peer in [partner] + [lax.rem(me + step, count) for step in range(2, count, 2)]:
            pl.semaphore_signal(
                barrier, inc=1, device_id={axis: peer}, device_id_type=pl.DeviceIdType.MESH
            )
        pl.semaphore_wait(barrier, count // 2)

        def send(item, source, block, peer, slot):
            copy = pltpu.make_async_remote_copy(
                src_ref=source,
                dst_ref=block_view(results[item], ROWS, block, count),
                send_sem=send_sem.at[item, slot],
                recv_sem=recv_sem.at[item, slot],
                device_id={axis: peer},
                device_id_type=pl.DeviceIdType.MESH,
            )
            copy.start()
            return copy

        far, near, own = [], [], []
        for item in range(number):
            for step in range(2, count, 2):
                peer = lax.rem(me + step, count)
                far.append((item, step, send(item, sources[item], me, peer, step)))
        for item in range(number):
            near.append(send(item, sources[item], me, partner, 1))
            own.append(
                pltpu.make_async_copy(
                    sources[item], block_view(results[item], ROWS, me, count), own_sem.at[item]
                )
            )
            own[-1].start()
        for item, step, copy in far:
            copy.wait_recv()
            origin = lax.rem(me - step + count, count)
            block = block_view(results[item], ROWS, origin, count)
            near.append(send(item, block, origin, partner, step + 1))
        for item, step, copy in far:
            copy.wait_send()
        for copy in near + own:
            copy.wait()

    return pl.pallas_call(
        kernel,
        out_shape=shapes,
        in_specs=[pl.BlockSpec(memory_space=pl.ANY)] * number,
        out_specs=[pl.BlockSpec(memory_space=pl.ANY)] * number,
        scratch_shapes=[
            pltpu.SemaphoreType.DMA((number, count)),
            pltpu.SemaphoreType.DMA((number, count)),
            pltpu.SemaphoreType.DMA((number,)),
        ],
        compiler_params=pltpu.CompilerParams(
            collective_id=collective_id, has_side_effects=True, vmem_limit_bytes=1 << 20
        ),
        cost_estimate=pl.CostEstimate(flops=0, bytes_accessed=COMM_BYTES, transcendentals=0),
    )(*arrays)


def chip_scatter(total, axis, collective_id):
    count = lax.axis_size(axis)
    chips = count // 2
    rows, cols = total.shape[0] // count, total.shape[1]
    shape = (chips * rows, cols)

    def kernel(total_ref, result, handed, sums, near_send, near_recv, far_send, far_recv):
        me = lax.axis_index(axis)
        core = lax.rem(me, 2)
        chip = lax.div(me, 2)
        partner = me + 1 - 2 * core
        barrier = pltpu.get_barrier_semaphore()
        for peer in [partner] + [lax.rem(me + step, count) for step in range(2, count, 2)]:
            pl.semaphore_signal(
                barrier, inc=1, device_id={axis: peer}, device_id_type=pl.DeviceIdType.MESH
            )
        pl.semaphore_wait(barrier, chips)
        order = list(range(1, chips)) + [0]
        near, far = [], []
        for step in order:
            target = lax.rem(chip + step, chips)
            copy = pltpu.make_async_remote_copy(
                src_ref=block_view(total_ref, ROWS, 2 * target + 1 - core, count),
                dst_ref=handed.at[pl.ds(step * rows, rows), :],
                send_sem=near_send.at[step],
                recv_sem=near_recv.at[step],
                device_id={axis: partner},
                device_id_type=pl.DeviceIdType.MESH,
            )
            copy.start()
            near.append(copy)
        for step, arrived in zip(order, near):
            arrived.wait_recv()
            target = lax.rem(chip + step, chips)
            place = pl.ds(step * rows, rows)
            own = block_view(total_ref, ROWS, 2 * target + core, count)[...]
            pair = own.astype(jnp.float32) + handed[place, :].astype(jnp.float32)
            if step == 0:
                result[pl.ds(pl.multiple_of(chip * rows, rows), rows), :] = pair.astype(result.dtype)
                continue
            sums[place, :] = pair.astype(sums.dtype)
            copy = pltpu.make_async_remote_copy(
                src_ref=sums.at[place, :],
                dst_ref=block_view(result, ROWS, chip, chips),
                send_sem=far_send.at[step],
                recv_sem=far_recv.at[step],
                device_id={axis: 2 * target + core},
                device_id_type=pl.DeviceIdType.MESH,
            )
            copy.start()
            far.append(copy)
        for copy in near:
            copy.wait_send()
        for copy in far:
            copy.wait()

    return pl.pallas_call(
        kernel,
        out_shape=jax.ShapeDtypeStruct(shape, total.dtype),
        in_specs=[pl.BlockSpec(memory_space=pltpu.VMEM)],
        out_specs=pl.BlockSpec(memory_space=pltpu.VMEM),
        scratch_shapes=[
            pltpu.VMEM(shape, total.dtype),
            pltpu.VMEM(shape, total.dtype),
            pltpu.SemaphoreType.DMA((chips,)),
            pltpu.SemaphoreType.DMA((chips,)),
            pltpu.SemaphoreType.DMA((chips,)),
            pltpu.SemaphoreType.DMA((chips,)),
        ],
        compiler_params=pltpu.CompilerParams(
            collective_id=collective_id, has_side_effects=True, vmem_limit_bytes=8 << 20
        ),
        cost_estimate=pl.CostEstimate(flops=0, bytes_accessed=COMM_BYTES, transcendentals=0),
    )(total)


def sum_blocks(received, count):
    rows = received.shape[0] // count
    total = received[:rows].astype(jnp.float32)
    for index in range(1, count):
        total = total + received[index * rows : (index + 1) * rows].astype(jnp.float32)
    return total


def product(left, right, left_dim, right_dim):
    return lax.dot_general(
        left, right, (((left_dim,), (right_dim,)), ((), ())), preferred_element_type=jnp.float32
    )


def allowed_pairs(layout, length):
    block = jnp.arange(length, dtype=jnp.int32) // BLK
    spread = (block[:, None] == jnp.arange(layout.shape[0], dtype=jnp.int32)[None, :]).astype(
        jnp.bfloat16
    )
    chosen = product(spread, (layout > 0).astype(jnp.bfloat16), 1, 0).astype(jnp.bfloat16)
    chosen = lax.dot_general(
        chosen, spread, (((1,), (1,)), ((), ())), preferred_element_type=jnp.bfloat16
    )
    chosen = chosen > 0.5
    position = jnp.arange(length, dtype=jnp.int32)
    return pair_mask(position, position, chosen)


def head_body(
    fixed_point, incoming, norm_gain, query_weight, key_weight, value_weight, out_weight, layout
):
    local_rows, model_width = fixed_point.shape
    tensor_count = lax.axis_size("tensor")
    seq_count = lax.axis_size("seq")
    head_width = query_weight.shape[1]
    head_count = head_width // HEAD_DIM
    own_heads = head_count // seq_count
    seq_tokens = local_rows * tensor_count
    seq_length = seq_tokens * seq_count
    score_scale = HEAD_DIM ** (-0.5)
    head_shape = (seq_tokens, head_count, HEAD_DIM)
    point = fixed_point.astype(jnp.float32)
    inv_rms = lax.rsqrt(jnp.mean(point * point, axis=1, keepdims=True) + EPS)
    scaled = point * inv_rms
    normed = (norm_gain * scaled).astype(jnp.bfloat16)
    piece, cotangent_piece = chip_gather((normed, incoming), "tensor", 0)
    cosine_all, sine_all = rope_tables(jnp.arange(seq_length, dtype=jnp.int32))
    first = lax.axis_index("seq") * seq_tokens
    cosine = lax.dynamic_slice_in_dim(cosine_all, first, seq_tokens, 0)
    sine = lax.dynamic_slice_in_dim(sine_all, first, seq_tokens, 0)
    cosine_all, sine_all = cosine_all[:, 0], sine_all[:, 0]

    def project(weight):
        return jnp.dot(piece, weight, preferred_element_type=jnp.float32)

    def turned(weight):
        values = rotate(project(weight).reshape(head_shape), cosine, sine)
        return values.astype(jnp.bfloat16).reshape(seq_tokens, head_width)

    grad_first = product(cotangent_piece, out_weight, 1, 1).astype(jnp.bfloat16)
    queries, keys, values, grad_heads = exchange(
        (
            turned(query_weight),
            turned(key_weight),
            project(value_weight).astype(jnp.bfloat16),
            grad_first,
        ),
        ((COLS, ROWS),) * 4,
        "seq",
        1,
    )
    allowed = allowed_pairs(layout, seq_length)
    heads = []
    for head in range(own_heads):
        part = slice(head * HEAD_DIM, (head + 1) * HEAD_DIM)
        query, key, value = queries[:, part], keys[:, part], values[:, part]
        scores = jnp.where(allowed, product(query, key, 1, 1) * score_scale, MASKED)
        probs = jnp.exp(scores - jax.nn.logsumexp(scores, axis=1, keepdims=True))
        probs_low = probs.astype(jnp.bfloat16)
        attended = product(probs_low, value, 1, 0).astype(jnp.bfloat16).astype(jnp.float32)
        heads.append((part, query, key, value, probs, probs_low, attended))
    cotangent = incoming.astype(jnp.float32)
    adjoint = cotangent
    gain_term = jnp.zeros((model_width,), jnp.float32)
    for term_index in range(ITERS):
        base = 2 + 4 * term_index
        if term_index:
            (cotangent_piece,) = chip_gather((cotangent.astype(jnp.bfloat16),), "tensor", base)
            (grad_heads,) = exchange(
                (product(cotangent_piece, out_weight, 1, 1).astype(jnp.bfloat16),),
                ((COLS, ROWS),),
                "seq",
                base + 1,
            )
        grads = []
        for part, query, key, value, probs, probs_low, attended in heads:
            grad_low = grad_heads[:, part]
            delta = jnp.sum(grad_low.astype(jnp.float32) * attended, axis=1, keepdims=True)
            grad_probs = product(grad_low, value, 1, 1)
            grad_scores = (probs * (grad_probs - delta)).astype(jnp.bfloat16)
            grad_query = product(grad_scores, key, 1, 0) * score_scale
            grad_key = product(grad_scores, query, 0, 0) * score_scale
            grad_value = product(probs_low, grad_low, 0, 0)
            grads.append(
                (
                    rotate_back(grad_query, cosine_all, sine_all).astype(jnp.bfloat16),
                    rotate_back(grad_key, cosine_all, sine_all).astype(jnp.bfloat16),
                    grad_value.astype(jnp.bfloat16),
                )
            )
        query_low, key_low, value_low = exchange(
            tuple(jnp.concatenate(items, axis=1) for items in zip(*grads)),
            ((ROWS, COLS),) * 3,
            "seq",
            base + 2,
        )
        total = product(query_low, query_weight, 1, 1)
        total = total + product(key_low, key_weight, 1, 1)
        total = total + product(value_low, value_weight, 1, 1)
        received = chip_scatter(total.astype(jnp.bfloat16), "tensor", base + 3)
        grad_normed = sum_blocks(received, tensor_count // 2)
        gain_term = gain_term + jnp.sum(grad_normed * scaled, axis=0)
        weighted = norm_gain * grad_normed
        inner = jnp.sum(weighted * scaled, axis=1, keepdims=True)
        cotangent = inv_rms * (weighted - scaled * (inner / model_width))
        adjoint = adjoint + cotangent
    shape = (8, model_width // 8)
    for axis, collective_id in (("tensor", 2 + 4 * ITERS), ("seq", 3 + 4 * ITERS)):
        (received,) = exchange((gain_term.reshape(shape),), ((WHOLE, ROWS),), axis, collective_id)
        gain_term = jnp.sum(received.reshape(-1, *shape), axis=0).reshape(-1)
    return (adjoint, gain_term * seq_length ** (-0.5))


def solution(mesh):
    in_specs = (
        P(("seq", "tensor"), None),
        P(("seq", "tensor"), None),
        P(),
        P(None, "tensor"),
        P(None, "tensor"),
        P(None, "tensor"),
        P("tensor", None),
        P(),
    )
    out_specs = (P(("seq", "tensor"), None), P())
    whole_heads = mesh.shape["tensor"] * mesh.shape["seq"]

    def body(*arrays):
        heads = arrays[3].shape[1] * mesh.shape["tensor"] // HEAD_DIM
        even = mesh.shape["tensor"] % 2 == 0
        chosen = head_body if even and heads % whole_heads == 0 else ring_body
        return chosen(*arrays)

    return jax.shard_map(body, mesh=mesh, in_specs=in_specs, out_specs=out_specs, check_vma=False)
```
